32 devices in a mesh: cp: 32 (over z, y, x, core).
Axes of the slice: x: 2, y: 2, z: 4, core: 2. Of those that a mesh axis runs over, the one named last changes fastest.
Arguments:
- queries: bfloat16 [16384, 512], P('cp'), may hold values from -6 to 6
- keys: bfloat16 [16384, 128], P('cp'), may hold values from -6 to 6
- values: bfloat16 [16384, 128], P('cp'), may hold values from -6 to 6
- grad_out: bfloat16 [16384, 512], P('cp'), may hold values from -6 to 6
- selections: int32 [32, 2], P('cp'), may hold values from -1 to 30, as said below
Outputs:
- attended: bfloat16 [16384, 512], P('cp')
- grad_queries: bfloat16 [16384, 512], P('cp')
- grad_keys: bfloat16 [16384, 128], P('cp')
- grad_values: bfloat16 [16384, 128], P('cp')
The draws below stay inside these ranges and needn't reach their ends.
Inputs may be any that keep to these rules, and one draw needn't show every extreme that they name: `selections`: row b names two different blocks before block b; where block b has fewer than two earlier blocks, the missing entries are -1 (blocks 0 and 1 only).
All inputs are finite; a program needn't handle non-finite values.
Results may differ from the reference program's by a relative error of at most 0.015.
Values may be sent and summed in bfloat16 or wider, within the bound.
No kernel may reach another device: no remote copies, remote signals or barrier semaphores. Data moves between devices by JAX's collectives and lax.ppermute only.
A program may use at most 128 MiB of HBM per device.

```python
import jax
import jax.numpy as jnp
from jax import lax

HEADS = 4
HEAD_DIM = 128
BLK = 512
SEQ = 16384
NBLK = 32


def draw_queries(key, part):
    base = jnp.clip(jax.random.normal(jax.random.fold_in(key, 1), (SEQ, HEADS * HEAD_DIM), jnp.float32), -6.0, 6.0)
    return base.astype(jnp.bfloat16)


def draw_keys(key, part):
    base = jnp.clip(jax.random.normal(jax.random.fold_in(key, 2), (SEQ, HEAD_DIM), jnp.float32), -6.0, 6.0)
    return base.astype(jnp.bfloat16)


def draw_selections(key, part):
    block_ids = jnp.arange(NBLK, dtype=jnp.int32)
    first_pick = jax.random.randint(jax.random.fold_in(key, 11), (NBLK,), 0, jnp.maximum(block_ids, 1))
    second_pick = jax.random.randint(jax.random.fold_in(key, 12), (NBLK,), 0, jnp.maximum(block_ids - 1, 1))
    second_pick = second_pick + (second_pick >= first_pick).astype(jnp.int32)
    hot_pick = jax.random.randint(jax.random.fold_in(key, 13), (NBLK,), 0, 8)
    coin_flip = jax.random.randint(jax.random.fold_in(key, 14), (NBLK,), 0, 2)
    use_hot = (coin_flip == 1) & (block_ids > 8) & (hot_pick != first_pick)
    second_pick = jnp.where(use_hot, hot_pick, second_pick)
    last_row = block_ids == NBLK - 1
    first_pick = jnp.where(last_row, NBLK - 2, first_pick)
    second_pick = jnp.where(last_row, hot_pick, second_pick)
    first_pick = jnp.where(block_ids >= 1, first_pick, -1)
    second_pick = jnp.where(block_ids >= 2, second_pick, -1)
    return jnp.stack([first_pick, second_pick], axis=1).astype(jnp.int32)


def level_of(key, dims, split, low, high):
    def one(axis_at, blocks):
        heights = jax.random.uniform(jax.random.fold_in(jax.random.fold_in(key, 6), axis_at), (blocks,), jnp.float32, low / len(split), high / len(split))
        return jnp.repeat(jnp.exp(heights), dims[axis_at] // blocks).reshape((-1,) + (1,) * (len(dims) - axis_at - 1))

    gain = one(*split[0])
    for cut in split[1:]:
        gain = gain * one(*cut)
    return gain


def noise(own_key, dims, width, reach, split=(), held_as=jnp.bfloat16):
    values = jax.random.normal(own_key, dims, jnp.float32) * width
    if len(split) > 0:
        values = level_of(own_key, dims, split, -0.22, 0.18) * values
    return jnp.clip(values, min=-reach, max=reach).astype(held_as)


def setup_inputs(seed: int = 0) -> dict:
    streams_of = jax.random.split(jax.random.key(seed), 6)
    queries = draw_queries(jax.random.fold_in(streams_of[5], 71), 0)
    keys = draw_keys(jax.random.fold_in(streams_of[5], 71), 0)
    values = noise(streams_of[2], (SEQ, HEAD_DIM), 1.0, 6.0, ((0, 32),))
    grad_out = noise(streams_of[3], (SEQ, HEADS * HEAD_DIM), 1.0, 6.0, ((0, 32),))
    selections = draw_selections(jax.random.fold_in(streams_of[5], 71), 0)
    return dict(queries=queries, keys=keys, values=values, grad_out=grad_out, selections=selections)


masked_value = -1e30


def key_mask(chosen):
    rows_at = lax.broadcasted_iota(jnp.int32, (BLK, BLK), 0)
    cols_at = lax.broadcasted_iota(jnp.int32, (BLK, BLK), 1)
    causal = cols_at <= rows_at
    first_ok = jnp.broadcast_to(chosen[0] >= 0, (BLK, BLK))
    second_ok = jnp.broadcast_to(chosen[1] >= 0, (BLK, BLK))
    return jnp.concatenate([causal, first_ok, second_ok], axis=1)


def block_grads(query_rows, block_keys, block_values, grad_rows, allowed):
    score_scale = HEAD_DIM ** -0.5
    query_heads = query_rows.reshape(BLK, HEADS, HEAD_DIM).astype(jnp.float32)
    keys_wide = block_keys.astype(jnp.float32)
    values_wide = block_values.astype(jnp.float32)
    scores = jnp.einsum("qhd,kd->hqk", query_heads, keys_wide) * score_scale
    scores = jnp.where(allowed[None], scores, masked_value)
    row_max = jnp.max(scores, axis=-1, keepdims=True)
    exponent = jnp.exp(scores - row_max)
    weights = exponent / jnp.sum(exponent, axis=-1, keepdims=True)
    probs_low = weights.astype(jnp.bfloat16).astype(jnp.float32)
    attended = jnp.einsum("hqk,kd->qhd", probs_low, values_wide).astype(jnp.bfloat16).reshape(BLK, HEADS * HEAD_DIM)
    grad_heads = grad_rows.reshape(BLK, HEADS, HEAD_DIM).astype(jnp.float32)
    grad_probs = jnp.einsum("qhd,kd->hqk", grad_heads, values_wide)
    inner_sum = jnp.sum(weights * grad_probs, axis=-1, keepdims=True)
    grad_scores = (weights * (grad_probs - inner_sum)).astype(jnp.bfloat16).astype(jnp.float32)
    grad_query = (jnp.einsum("hqk,kd->qhd", grad_scores, keys_wide) * score_scale).astype(jnp.bfloat16)
    grad_k = jnp.einsum("hqk,qhd->kd", grad_scores, query_heads) * score_scale
    grad_v = jnp.einsum("hqk,qhd->kd", probs_low, grad_heads)
    return attended, grad_query.reshape(BLK, HEADS * HEAD_DIM), grad_k, grad_v


def take_rows(array, start):
    return lax.dynamic_slice_in_dim(array, start, BLK, 0)


def reference(queries, keys, values, grad_out, selections):
    def advance(totals, block_id):
        grad_keys, grad_values = totals
        start = (block_id * BLK).astype(jnp.int32)
        chosen = selections[block_id]
        starts = [start, (jnp.maximum(chosen[0], 0) * BLK).astype(jnp.int32), (jnp.maximum(chosen[1], 0) * BLK).astype(jnp.int32)]
        block_keys = jnp.concatenate([take_rows(keys, s) for s in starts], axis=0)
        block_values = jnp.concatenate([take_rows(values, s) for s in starts], axis=0)
        attended, grad_query, grad_k, grad_v = block_grads(take_rows(queries, start), block_keys, block_values, take_rows(grad_out, start), key_mask(chosen))
        for member in range(3):
            begin = starts[member]
            grad_keys = lax.dynamic_update_slice_in_dim(grad_keys, take_rows(grad_keys, begin) + grad_k[member * BLK:(member + 1) * BLK], begin, 0)
            grad_values = lax.dynamic_update_slice_in_dim(grad_values, take_rows(grad_values, begin) + grad_v[member * BLK:(member + 1) * BLK], begin, 0)
        return (grad_keys, grad_values), (attended, grad_query)

    zeros_init = jnp.zeros((SEQ, HEAD_DIM), jnp.float32)
    (grad_keys, grad_values), (attended, grad_queries) = lax.scan(advance, (zeros_init, zeros_init), jnp.arange(NBLK, dtype=jnp.int32))
    return (attended.reshape(SEQ, HEADS * HEAD_DIM), grad_queries.reshape(SEQ, HEADS * HEAD_DIM), grad_keys.astype(jnp.bfloat16), grad_values.astype(jnp.bfloat16))
```

```python
import functools

import jax
import jax.numpy as jnp
from jax import lax
from jax.experimental import pallas as pl
from jax.experimental.pallas import tpu as pltpu
from jax.sharding import PartitionSpec as P

HEADS = 4
HEAD_DIM = 128
BLK = 512
SUB = 8
DIGIT = 128
SCALE = HEAD_DIM ** (-0.5)
LOG2_SCALE = SCALE * 1.4426950408889634
MASKED = -1e30

f32 = jnp.float32
bf16 = jnp.bfloat16


def dot(a, b):
    return lax.dot_general(a, b, (((1,), (0,)), ((), ())), preferred_element_type=f32)


def vmem():
    return pl.BlockSpec(memory_space=pltpu.VMEM)


def smem():
    return pl.BlockSpec(memory_space=pltpu.SMEM)


def params(mib=40):
    return pltpu.CompilerParams(vmem_limit_bytes=mib * 1024 * 1024)


def cost(flops, trans=0, nbytes=1024):
    return pl.CostEstimate(flops=flops, transcendentals=trans, bytes_accessed=nbytes)


def pack_kernel(sel_ref, keys_ref, values_ref, out_ref):
    parts, rows, width = out_ref.shape
    rows = rows - SUB
    half = parts // 2
    out_ref[:half, :rows, :] = keys_ref[...].reshape(half, rows, width)
    out_ref[half:, :rows, :] = values_ref[...].reshape(half, rows, width)
    lane = lax.broadcasted_iota(jnp.int32, (SUB, width), 1)
    ids = jnp.zeros((SUB, width), jnp.int32)
    for slot in range(2):
        number = sel_ref[0, slot] + 1
        ids = jnp.where(lane == 2 * slot, lax.shift_right_logical(number, 7), ids)
        ids = jnp.where(lane == 2 * slot + 1, number & (DIGIT - 1), ids)
    tail = ids.astype(f32).astype(bf16)
    out_ref[:, rows:, :] = jnp.broadcast_to(tail[None], (parts, SUB, width))


def request_of(ids_ref, reader, slot):
    return ids_ref[reader, 2 * slot] * DIGIT + ids_ref[reader, 2 * slot + 1] - 1


def gather_kernel(held_ref, out_ref, ids_ref, ids_smem, sem):
    readers, _, rows, width = out_ref.shape
    tail = held_ref[:, rows:, :].astype(f32)
    ids_ref[...] = jnp.max(tail, axis=1).astype(jnp.int32)
    copy = pltpu.make_async_copy(ids_ref, ids_smem, sem)
    copy.start()
    copy.wait()

    def one(reader, carry):
        for slot in range(2):
            block = jnp.maximum(request_of(ids_smem, reader, slot), 0)
            out_ref[reader, slot] = held_ref[block, :rows, :]
        return carry

    lax.fori_loop(0, readers, one, 0, unroll=8)


def pre_kernel(queries_ref, grad_ref, keys_ref, values_ref, qt_ref, gt_ref, stats_ref):
    keys = keys_ref[...]
    values = values_ref[...]
    key_at = lax.broadcasted_iota(jnp.int32, (BLK, BLK), 0)
    query_at = lax.broadcasted_iota(jnp.int32, (BLK, BLK), 1)
    causal = key_at <= query_at
    for h in range(HEADS):
        cols = slice(h * HEAD_DIM, (h + 1) * HEAD_DIM)
        qt = queries_ref[:, cols].T
        gt = grad_ref[:, cols].T
        qt_ref[h] = qt
        gt_ref[h] = gt
        scores = jnp.where(causal, dot(keys, qt), MASKED)
        top = jnp.max(scores, axis=0, keepdims=True)
        weight = jnp.exp2(scores * LOG2_SCALE - top * LOG2_SCALE)
        stats_ref[h, 0:1, :] = top
        stats_ref[h, 1:2, :] = jnp.sum(weight, axis=0, keepdims=True)
        stats_ref[h, 2:3, :] = jnp.sum(weight * dot(values, gt), axis=0, keepdims=True)


def slot_terms(sel_ref, slot):
    ok = sel_ref[0, slot] >= 0
    return jnp.where(ok, 1.0, 0.0), jnp.where(ok, 0.0, 1e30), jnp.where(ok, 0.0, MASKED)


def main_kernel(sel_ref, fetched_ref, qt_ref, gt_ref, queries_ref, grad_ref, own_ref, out_ref, stats_ref):
    parts, _, rows, width = fetched_ref.shape
    half = parts // 2
    keys = [fetched_ref[:half, s].reshape(BLK, width) for s in range(2)]
    values = [fetched_ref[half:, s].reshape(BLK, width) for s in range(2)]
    terms = [slot_terms(sel_ref, s) for s in range(2)]
    grad_k = [None, None]
    grad_v = [None, None]
    for h in range(HEADS):
        cols = slice(h * HEAD_DIM, (h + 1) * HEAD_DIM)
        qt = qt_ref[h]
        gt = gt_ref[h]
        q_h = queries_ref[:, cols]
        g_h = grad_ref[:, cols]
        top0 = own_ref[h, 0:1, :]
        scores = [dot(keys[s], qt) for s in range(2)]
        top = top0
        for s in range(2):
            _, _, low = terms[s]
            keep, _, _ = terms[s]
            top = jnp.maximum(top, jnp.max(scores[s], axis=0, keepdims=True) * keep + low)
        base = top * LOG2_SCALE
        alpha = jnp.exp2(top0 * LOG2_SCALE - base)
        total = own_ref[h, 1:2, :] * alpha
        inner = own_ref[h, 2:3, :] * alpha
        weight = []
        for s in range(2):
            keep, high, _ = terms[s]
            w = jnp.exp2(scores[s] * (keep * LOG2_SCALE) - (base * keep + high))
            weight.append(w)
            total = total + jnp.sum(w, axis=0, keepdims=True)
        inverse = 1.0 / total
        inner = inner * inverse
        grads = []
        for s in range(2):
            weight[s] = weight[s] * inverse
            grads.append(dot(values[s], gt))
            inner = inner + jnp.sum(weight[s] * grads[s], axis=0, keepdims=True)
        for s in range(2):
            dv = dot(weight[s].astype(bf16), g_h)
            grad_v[s] = dv if grad_v[s] is None else grad_v[s] + dv
            ds = (weight[s] * (grads[s] - inner)).astype(bf16)
            dk = dot(ds, q_h)
            grad_k[s] = dk if grad_k[s] is None else grad_k[s] + dk
        stats_ref[h, 0:1, :] = base
        stats_ref[h, 1:2, :] = inverse
        stats_ref[h, 2:3, :] = inner
    for s in range(2):
        out_ref[:half, s] = (grad_k[s] * SCALE).astype(bf16).reshape(half, rows, width)
        out_ref[half:, s] = grad_v[s].astype(bf16).reshape(half, rows, width)


def selected_kernel(sel_ref, fetched_ref, qt_ref, gt_ref, stats_ref, att_ref, dq_ref):
    parts, _, rows, width = fetched_ref.shape
    half = parts // 2
    terms = [slot_terms(sel_ref, s) for s in range(2)]
    keys = [fetched_ref[:half, s].reshape(BLK, width) for s in range(2)]
    values = [fetched_ref[half:, s].reshape(BLK, width) for s in range(2)]
    keys_t = [k.T for k in keys]
    values_t = [v.T for v in values]
    for h in range(HEADS):
        base = stats_ref[h, 0:1, :]
        inverse = stats_ref[h, 1:2, :]
        inner = stats_ref[h, 2:3, :]
        att = None
        dq = None
        for s in range(2):
            keep, high, _ = terms[s]
            scores = dot(keys[s], qt_ref[h])
            w = jnp.exp2(scores * (keep * LOG2_SCALE) - (base * keep + high)) * inverse
            ds = (w * (dot(values[s], gt_ref[h]) - inner)).astype(bf16)
            att_s = dot(values_t[s], w.astype(bf16))
            dq_s = dot(keys_t[s], ds)
            att = att_s if att is None else att + att_s
            dq = dq_s if dq is None else dq + dq_s
        att_ref[h] = att
        dq_ref[h] = dq


def own_kernel(keys_ref, values_ref, qt_ref, gt_ref, queries_ref, grad_ref, stats_ref, att_ref, dq_ref, att_out, dq_out, own_out):
    keys = keys_ref[...]
    values = values_ref[...]
    keys_t = keys.T
    values_t = values.T
    key_at = lax.broadcasted_iota(jnp.int32, (BLK, BLK), 0)
    query_at = lax.broadcasted_iota(jnp.int32, (BLK, BLK), 1)
    causal = key_at <= query_at
    grad_k = None
    grad_v = None
    for h in range(HEADS):
        cols = slice(h * HEAD_DIM, (h + 1) * HEAD_DIM)
        base = stats_ref[h, 0:1, :]
        inverse = stats_ref[h, 1:2, :]
        inner = stats_ref[h, 2:3, :]
        scores = jnp.where(causal, dot(keys, qt_ref[h]) * LOG2_SCALE, MASKED)
        w = jnp.exp2(scores - base) * inverse
        low = w.astype(bf16)
        ds = (w * (dot(values, gt_ref[h]) - inner)).astype(bf16)
        att = att_ref[h] + dot(values_t, low)
        dq = (dq_ref[h] + dot(keys_t, ds)) * SCALE
        att_out[:, cols] = att.T.astype(bf16)
        dq_out[:, cols] = dq.T.astype(bf16)
        dv = dot(low, grad_ref[:, cols])
        dk = dot(ds, queries_ref[:, cols])
        grad_v = dv if grad_v is None else grad_v + dv
        grad_k = dk if grad_k is None else grad_k + dk
    own_out[:BLK, :] = grad_k * SCALE
    own_out[BLK:, :] = grad_v


def sum_kernel(ids_ref, received_ref, out_ref, acc_ref):
    readers = received_ref.shape[0]
    acc_ref[...] = jnp.zeros(acc_ref.shape, f32)

    def one(reader, carry):
        for slot in range(2):
            block = jnp.maximum(request_of(ids_ref, reader, slot), 0)
            acc_ref[block] = acc_ref[block] + received_ref[reader, slot].astype(f32)
        return carry

    lax.fori_loop(0, readers, one, 0, unroll=8)
    out_ref[...] = acc_ref[...].astype(bf16)


def final_kernel(returned_ref, own_ref, dk_ref, dv_ref):
    parts, rows, width = returned_ref.shape
    half = parts // 2
    dk_ref[...] = (returned_ref[:half].reshape(BLK, width).astype(f32) + own_ref[:BLK, :]).astype(bf16)
    dv_ref[...] = (returned_ref[half:].reshape(BLK, width).astype(f32) + own_ref[BLK:, :]).astype(bf16)


def exchange(array):
    return lax.all_to_all(array, "cp", split_axis=0, concat_axis=0, tiled=True)


def body(queries, keys, values, grad_out, selections):
    parts = lax.axis_size("cp")
    width = keys.shape[1]
    rows = 2 * BLK // parts
    shape = jax.ShapeDtypeStruct
    unit = 2 * HEADS * BLK * BLK * HEAD_DIM

    packed = pl.pallas_call(
        pack_kernel,
        out_shape=shape((parts, rows + SUB, width), bf16),
        in_specs=[smem(), vmem(), vmem()],
        out_specs=vmem(),
        compiler_params=params(),
        cost_estimate=cost(1000000),
        name="pack",
    )(selections, keys, values)
    held = exchange(packed)
    heads_t = shape((HEADS, HEAD_DIM, BLK), bf16)
    stats = shape((HEADS, SUB, BLK), f32)
    q_t, g_t, own_stats = pl.pallas_call(
        pre_kernel,
        out_shape=(heads_t, heads_t, stats),
        in_specs=[vmem()] * 4,
        out_specs=(vmem(),) * 3,
        compiler_params=params(),
        cost_estimate=cost(2 * unit, HEADS * BLK * BLK),
        name="pre",
    )(queries, grad_out, keys, values)
    outgoing, ids = pl.pallas_call(
        gather_kernel,
        out_shape=(shape((parts, 2, rows, width), bf16), shape((parts, width), jnp.int32)),
        in_specs=[vmem()],
        out_specs=(vmem(), vmem()),
        scratch_shapes=[pltpu.SMEM((parts, width), jnp.int32), pltpu.SemaphoreType.DMA],
        compiler_params=params(),
        cost_estimate=cost(1000000),
        name="gather",
    )(held)
    fetched = exchange(outgoing)
    partial, full_stats = pl.pallas_call(
        main_kernel,
        out_shape=(shape((parts, 2, rows, width), bf16), stats),
        in_specs=[smem()] + [vmem()] * 6,
        out_specs=(vmem(), vmem()),
        compiler_params=params(56),
        cost_estimate=cost(8 * unit, 2 * HEADS * BLK * BLK),
        name="main",
    )(selections, fetched, q_t, g_t, queries, grad_out, own_stats)
    received = exchange(partial)
    acc_t = shape((HEADS, HEAD_DIM, BLK), f32)
    att_t, dq_t = pl.pallas_call(
        selected_kernel,
        out_shape=(acc_t, acc_t),
        in_specs=[smem()] + [vmem()] * 4,
        out_specs=(vmem(), vmem()),
        compiler_params=params(56),
        cost_estimate=cost(8 * unit, 2 * HEADS * BLK * BLK),
        name="selected",
    )(selections, fetched, q_t, g_t, full_stats)
    summed = pl.pallas_call(
        sum_kernel,
        out_shape=shape((parts, rows, width), bf16),
        in_specs=[smem(), vmem()],
        out_specs=vmem(),
        scratch_shapes=[pltpu.VMEM((parts, rows, width), f32)],
        compiler_params=params(),
        cost_estimate=cost(1000000),
        name="sum",
    )(ids, received)
    returned = exchange(summed)
    attended, grad_queries, own_grads = pl.pallas_call(
        own_kernel,
        out_shape=(shape((BLK, HEADS * HEAD_DIM), bf16), shape((BLK, HEADS * HEAD_DIM), bf16), shape((2 * BLK, width), f32)),
        in_specs=[vmem()] * 9,
        out_specs=(vmem(),) * 3,
        compiler_params=params(56),
        cost_estimate=cost(6 * unit, HEADS * BLK * BLK),
        name="own",
    )(keys, values, q_t, g_t, queries, grad_out, full_stats, att_t, dq_t)
    grad_keys, grad_values = pl.pallas_call(
        final_kernel,
        out_shape=(shape((BLK, width), bf16), shape((BLK, width), bf16)),
        in_specs=[vmem(), vmem()],
        out_specs=(vmem(), vmem()),
        compiler_params=params(),
        cost_estimate=cost(1000000),
        name="final",
    )(returned, own_grads)
    return attended, grad_queries, grad_keys, grad_values


def solution(mesh):
    in_specs = (P("cp", None), P("cp", None), P("cp", None), P("cp", None), P("cp", None))
    out_specs = (P("cp", None), P("cp", None), P("cp", None), P("cp", None))
    return jax.shard_map(body, mesh=mesh, in_specs=in_specs, out_specs=out_specs, check_vma=False)
```

```python
import jax
import jax.numpy as jnp
from jax import lax
from jax.experimental import pallas as pl
from jax.experimental.pallas import tpu as pltpu
from jax.sharding import PartitionSpec as P


HEADS = 4
HEAD_DIM = 128
BLK = 512
SUB = 8
DIGIT = 128
SCALE = HEAD_DIM ** (-0.5)
LOG2_SCALE = SCALE * 1.4426950408889634
MASKED = -1e30

WHOLE_VMEM = 67_000_000

f32 = jnp.float32
bf16 = jnp.bfloat16


def dot(a, b):
    return lax.dot_general(a, b, (((1,), (0,)), ((), ())), preferred_element_type=f32)


def vmem():
    return pl.BlockSpec(memory_space=pltpu.VMEM)


def smem():
    return pl.BlockSpec(memory_space=pltpu.SMEM)


def hbm():
    return pl.BlockSpec(memory_space=pltpu.HBM)


def params(mib=16):
    return pltpu.CompilerParams(vmem_limit_bytes=mib * 1024 * 1024)


def cost(flops, trans=0, nbytes=1024):
    return pl.CostEstimate(flops=flops, transcendentals=trans, bytes_accessed=nbytes)


def pack_kernel(sel_ref, keys_ref, values_ref, out_ref, sel_smem, sems):
    parts, rows, width = out_ref.shape
    rows = rows - SUB
    half = parts // 2
    copies = [
        pltpu.make_async_copy(keys_ref, out_ref.at[:half, :rows, :], sems.at[0]),
        pltpu.make_async_copy(values_ref, out_ref.at[half:, :rows, :], sems.at[1]),
    ]
    chosen = pltpu.make_async_copy(sel_ref, sel_smem, sems.at[2])
    chosen.start()
    for copy in copies:
        copy.start()
    chosen.wait()
    lane = lax.broadcasted_iota(jnp.int32, (SUB, width), 1)
    ids = jnp.zeros((SUB, width), jnp.int32)
    for slot in range(2):
        number = sel_smem[0, slot] + 1
        ids = jnp.where(lane == 2 * slot, lax.shift_right_logical(number, 7), ids)
        ids = jnp.where(lane == 2 * slot + 1, number & (DIGIT - 1), ids)
    tail = ids.astype(f32).astype(bf16)
    out_ref[:, rows:, :] = jnp.broadcast_to(tail[None], (parts, SUB, width))
    for copy in copies:
        copy.wait()


def request_of(ids_ref, reader, slot):
    return ids_ref[reader, 2 * slot] * DIGIT + ids_ref[reader, 2 * slot + 1] - 1


def gather_kernel(held_ref, out_ref, ids_ref, ids_smem, sem):
    readers, _, rows, _ = out_ref.shape
    tail = held_ref[:, rows:, :].astype(f32)
    ids_ref[...] = jnp.max(tail, axis=1).astype(jnp.int32)
    copy = pltpu.make_async_copy(ids_ref, ids_smem, sem)
    copy.start()
    copy.wait()

    def one(reader, carry):
        for slot in range(2):
            block = jnp.maximum(request_of(ids_smem, reader, slot), 0)
            out_ref[reader, slot] = held_ref[block, :rows, :]
        return carry

    lax.fori_loop(0, readers, one, 0, unroll=8)


def pre_kernel(sel_ref, queries_ref, grad_ref, keys_ref, values_ref, qt_ref, gt_ref, stats_ref):
    keys = keys_ref[...]
    values = values_ref[...]
    key_at = lax.broadcasted_iota(jnp.int32, (BLK, BLK), 0)
    query_at = lax.broadcasted_iota(jnp.int32, (BLK, BLK), 1)
    causal = key_at <= query_at
    for h in range(HEADS):
        cols = slice(h * HEAD_DIM, (h + 1) * HEAD_DIM)
        qt = queries_ref[:, cols].T
        gt = grad_ref[:, cols].T
        qt_ref[h] = qt
        gt_ref[h] = gt
        scores = jnp.where(causal, dot(keys, qt), MASKED)
        top = jnp.max(scores, axis=0, keepdims=True)
        weight = jnp.exp2(scores * LOG2_SCALE - top * LOG2_SCALE)
        stats_ref[h, 0:1, :] = top
        stats_ref[h, 1:2, :] = jnp.sum(weight, axis=0, keepdims=True)
        stats_ref[h, 2:3, :] = jnp.sum(weight * dot(values, gt), axis=0, keepdims=True)
        for slot in range(2):
            keep = jnp.where(sel_ref[0, slot] >= 0, 1.0, 0.0)
            stats_ref[h, 3 + slot : 4 + slot, :] = jnp.full((1, BLK), keep, f32)


def slot_terms(stats_ref, slot):
    keep = stats_ref[0, 3 + slot : 4 + slot, :]
    return keep, (1.0 - keep) * 1e30


def main_kernel(
    fetched_ref, qt_ref, gt_ref, queries_ref, grad_ref, own_ref, out_ref, stats_ref, score_ref, gp_ref, low_ref, ds_ref
):
    parts, _, rows, width = fetched_ref.shape
    half = parts // 2
    step = 128
    count = 2 * BLK // step
    keys = [fetched_ref[:half, s].reshape(BLK, width) for s in range(2)]
    values = [fetched_ref[half:, s].reshape(BLK, width) for s in range(2)]
    terms = [slot_terms(own_ref, s) for s in range(2)]

    def at(c):
        return slice(c * step, (c + 1) * step)

    def piece(blocks, c):
        s, first = divmod(c * step, BLK)
        return blocks[s][first : first + step, :]

    def fold(x, reduce):
        return reduce(x.reshape(step // SUB, SUB, BLK), axis=0)

    for h in range(HEADS):
        wide = slice(h * BLK, (h + 1) * BLK)
        buf = h % 2
        qt = qt_ref[h]
        gt = gt_ref[h]
        tops = [None, None]
        for c in range(count):
            s = c * step // BLK
            x = dot(piece(keys, c), qt)
            score_ref[buf, at(c), :] = x
            m = fold(x, jnp.max)
            tops[s] = m if tops[s] is None else jnp.maximum(tops[s], m)
        for c in range(count):
            gp_ref[buf, at(c), :] = dot(piece(values, c), gt)
        top0 = own_ref[h, 0:1, :]
        top = top0
        for s in range(2):
            keep, far = terms[s]
            top = jnp.maximum(top, jnp.max(tops[s], axis=0, keepdims=True) * keep - far)
        base = top * LOG2_SCALE
        alpha = jnp.exp2(top0 * LOG2_SCALE - base)
        total8 = None
        inner8 = None
        for c in range(count):
            keep, far = terms[c * step // BLK]
            w = jnp.exp2(score_ref[buf, at(c), :] * (keep * LOG2_SCALE) - (base * keep + far))
            score_ref[buf, at(c), :] = w
            t = fold(w, jnp.sum)
            i = fold(w * gp_ref[buf, at(c), :], jnp.sum)
            total8 = t if total8 is None else total8 + t
            inner8 = i if inner8 is None else inner8 + i
        total = own_ref[h, 1:2, :] * alpha + jnp.sum(total8, axis=0, keepdims=True)
        inverse = 1.0 / total
        inner = (own_ref[h, 2:3, :] * alpha + jnp.sum(inner8, axis=0, keepdims=True)) * inverse
        for c in range(count):
            w = score_ref[buf, at(c), :] * inverse
            low_ref[at(c), wide] = w.astype(bf16)
            ds_ref[at(c), wide] = (w * (gp_ref[buf, at(c), :] - inner)).astype(bf16)
        stats_ref[h, 0:1, :] = base
        stats_ref[h, 1:2, :] = inverse
        stats_ref[h, 2:3, :] = inner
        stats_ref[h, 3:5, :] = own_ref[h, 3:5, :]
    q_tall = jnp.concatenate([queries_ref[:, h * HEAD_DIM : (h + 1) * HEAD_DIM] for h in range(HEADS)], axis=0)
    g_tall = jnp.concatenate([grad_ref[:, h * HEAD_DIM : (h + 1) * HEAD_DIM] for h in range(HEADS)], axis=0)
    for s in range(2):
        block = slice(s * BLK, (s + 1) * BLK)
        out_ref[half:, s] = dot(low_ref[block, :], g_tall).astype(bf16).reshape(half, rows, width)
        out_ref[:half, s] = (dot(ds_ref[block, :], q_tall) * SCALE).astype(bf16).reshape(half, rows, width)


def selected_kernel(fetched_ref, qt_ref, gt_ref, stats_ref, att_ref, dq_ref):
    parts, _, _, width = fetched_ref.shape
    half = parts // 2
    terms = [slot_terms(stats_ref, s) for s in range(2)]
    keys = [fetched_ref[:half, s].reshape(BLK, width) for s in range(2)]
    values = [fetched_ref[half:, s].reshape(BLK, width) for s in range(2)]
    keys_t = [k.T for k in keys]
    values_t = [v.T for v in values]
    for h in range(HEADS):
        base = stats_ref[h, 0:1, :]
        inverse = stats_ref[h, 1:2, :]
        inner = stats_ref[h, 2:3, :]
        att = None
        dq = None
        for s in range(2):
            keep, far = terms[s]
            scores = dot(keys[s], qt_ref[h])
            w = jnp.exp2(scores * (keep * LOG2_SCALE) - (base * keep + far)) * inverse
            ds = (w * (dot(values[s], gt_ref[h]) - inner)).astype(bf16)
            att_s = dot(values_t[s], w.astype(bf16))
            dq_s = dot(keys_t[s], ds)
            att = att_s if att is None else att + att_s
            dq = dq_s if dq is None else dq + dq_s
        att_ref[h] = att
        dq_ref[h] = dq


def own_kernel(keys_ref, values_ref, qt_ref, gt_ref, queries_ref, grad_ref, stats_ref, att_ref, dq_ref, att_out, dq_out, own_out):
    keys = keys_ref[...]
    values = values_ref[...]
    keys_t = keys.T
    values_t = values.T
    key_at = lax.broadcasted_iota(jnp.int32, (BLK, BLK), 0)
    query_at = lax.broadcasted_iota(jnp.int32, (BLK, BLK), 1)
    causal = key_at <= query_at
    grad_k = None
    grad_v = None
    for h in range(HEADS):
        cols = slice(h * HEAD_DIM, (h + 1) * HEAD_DIM)
        base = stats_ref[h, 0:1, :]
        inverse = stats_ref[h, 1:2, :]
        inner = stats_ref[h, 2:3, :]
        scores = jnp.where(causal, dot(keys, qt_ref[h]) * LOG2_SCALE, MASKED)
        w = jnp.exp2(scores - base) * inverse
        low = w.astype(bf16)
        ds = (w * (dot(values, gt_ref[h]) - inner)).astype(bf16)
        att = att_ref[h] + dot(values_t, low)
        dq = (dq_ref[h] + dot(keys_t, ds)) * SCALE
        att_out[:, cols] = att.T.astype(bf16)
        dq_out[:, cols] = dq.T.astype(bf16)
        dv = dot(low, grad_ref[:, cols])
        dk = dot(ds, queries_ref[:, cols])
        grad_v = dv if grad_v is None else grad_v + dv
        grad_k = dk if grad_k is None else grad_k + dk
    own_out[:BLK, :] = grad_k * SCALE
    own_out[BLK:, :] = grad_v


def sum_kernel(ids_ref, received_ref, out_ref, acc_ref, ids_smem, sem):
    readers = received_ref.shape[0]
    copy = pltpu.make_async_copy(ids_ref, ids_smem, sem)
    copy.start()
    acc_ref[...] = jnp.zeros(acc_ref.shape, f32)
    copy.wait()

    def one(reader, carry):
        for slot in range(2):
            block = jnp.maximum(request_of(ids_smem, reader, slot), 0)
            acc_ref[block] = acc_ref[block] + received_ref[reader, slot].astype(f32)
        return carry

    lax.fori_loop(0, readers, one, 0, unroll=8)
    out_ref[...] = acc_ref[...].astype(bf16)


def final_kernel(returned_ref, own_ref, dk_ref, dv_ref):
    parts, _, width = returned_ref.shape
    half = parts // 2
    dk_ref[...] = (returned_ref[:half].reshape(BLK, width).astype(f32) + own_ref[:BLK, :]).astype(bf16)
    dv_ref[...] = (returned_ref[half:].reshape(BLK, width).astype(f32) + own_ref[BLK:, :]).astype(bf16)


def exchange(array):
    return lax.all_to_all(array, "cp", split_axis=0, concat_axis=0, tiled=True)


def body(queries, keys, values, grad_out, selections):
    parts = lax.axis_size("cp")
    width = keys.shape[1]
    rows = 2 * BLK // parts
    shape = jax.ShapeDtypeStruct
    unit = 2 * HEADS * BLK * BLK * HEAD_DIM

    packed = pl.pallas_call(
        pack_kernel,
        out_shape=shape((parts, rows + SUB, width), bf16),
        in_specs=[hbm(), hbm(), hbm()],
        out_specs=vmem(),
        scratch_shapes=[pltpu.SMEM((1, 2), jnp.int32), pltpu.SemaphoreType.DMA((3,))],
        compiler_params=pltpu.CompilerParams(vmem_limit_bytes=WHOLE_VMEM),
        cost_estimate=cost(1000000),
        name="pack",
    )(selections, keys.reshape(parts // 2, rows, width), values.reshape(parts // 2, rows, width))
    held = exchange(packed)
    heads_t = shape((HEADS, HEAD_DIM, BLK), bf16)
    stats = shape((HEADS, SUB, BLK), f32)
    q_t, g_t, own_stats = pl.pallas_call(
        pre_kernel,
        out_shape=(heads_t, heads_t, stats),
        in_specs=[smem()] + [vmem()] * 4,
        out_specs=(vmem(),) * 3,
        compiler_params=params(),
        cost_estimate=cost(2 * unit, HEADS * BLK * BLK),
        name="pre",
    )(selections, queries, grad_out, keys, values)
    outgoing, ids = pl.pallas_call(
        gather_kernel,
        out_shape=(shape((parts, 2, rows, width), bf16), shape((parts, width), jnp.int32)),
        in_specs=[vmem()],
        out_specs=(vmem(), vmem()),
        scratch_shapes=[pltpu.SMEM((parts, width), jnp.int32), pltpu.SemaphoreType.DMA],
        compiler_params=params(),
        cost_estimate=cost(1000000),
        name="gather",
    )(held)
    fetched = exchange(outgoing)
    partial, full_stats = pl.pallas_call(
        main_kernel,
        out_shape=(shape((parts, 2, rows, width), bf16), stats),
        in_specs=[vmem()] * 6,
        out_specs=(vmem(), vmem()),
        scratch_shapes=[
            pltpu.VMEM((2, 2 * BLK, BLK), f32),
            pltpu.VMEM((2, 2 * BLK, BLK), f32),
            pltpu.VMEM((2 * BLK, HEADS * BLK), bf16),
            pltpu.VMEM((2 * BLK, HEADS * BLK), bf16),
        ],
        compiler_params=params(28),
        cost_estimate=cost(8 * unit, 2 * HEADS * BLK * BLK),
        name="main",
    )(fetched, q_t, g_t, queries, grad_out, own_stats)
    received = exchange(partial)
    acc_t = shape((HEADS, HEAD_DIM, BLK), f32)
    att_t, dq_t = pl.pallas_call(
        selected_kernel,
        out_shape=(acc_t, acc_t),
        in_specs=[vmem()] * 4,
        out_specs=(vmem(), vmem()),
        compiler_params=params(28),
        cost_estimate=cost(8 * unit, 2 * HEADS * BLK * BLK),
        name="selected",
    )(fetched, q_t, g_t, full_stats)
    summed = pl.pallas_call(
        sum_kernel,
        out_shape=shape((parts, rows, width), bf16),
        in_specs=[vmem(), vmem()],
        out_specs=vmem(),
        scratch_shapes=[
            pltpu.VMEM((parts, rows, width), f32),
            pltpu.SMEM((parts, width), jnp.int32),
            pltpu.SemaphoreType.DMA,
        ],
        compiler_params=params(),
        cost_estimate=cost(1000000),
        name="sum",
    )(ids, received)
    returned = exchange(summed)
    attended, grad_queries, own_grads = pl.pallas_call(
        own_kernel,
        out_shape=(shape((BLK, HEADS * HEAD_DIM), bf16), shape((BLK, HEADS * HEAD_DIM), bf16), shape((2 * BLK, width), f32)),
        in_specs=[vmem()] * 9,
        out_specs=(vmem(),) * 3,
        compiler_params=params(28),
        cost_estimate=cost(6 * unit, HEADS * BLK * BLK),
        name="own",
    )(keys, values, q_t, g_t, queries, grad_out, full_stats, att_t, dq_t)
    grad_keys, grad_values = pl.pallas_call(
        final_kernel,
        out_shape=(shape((BLK, width), bf16), shape((BLK, width), bf16)),
        in_specs=[vmem(), vmem()],
        out_specs=(vmem(), vmem()),
        compiler_params=params(),
        cost_estimate=cost(1000000),
        name="final",
    )(returned, own_grads)
    return attended, grad_queries, grad_keys, grad_values


def solution(mesh):
    in_specs = (P("cp", None), P("cp", None), P("cp", None), P("cp", None), P("cp", None))
    out_specs = (P("cp", None), P("cp", None), P("cp", None), P("cp", None))
    return jax.shard_map(body, mesh=mesh, in_specs=in_specs, out_specs=out_specs, check_vma=False)
```
